32 devices in a mesh: grp: 4 (over z), dom: 8 (over y, x, core).
Axes of the slice: x: 2, y: 2, z: 4, core: 2. Of those that a mesh axis runs over, the one named last changes fastest.
Arguments:
- fluid_start: float32 [4, 256, 96, 128], P('grp', 'dom'), may hold values from -6 to 6
- fluid_rate: float32 [4, 256, 96, 128], P('grp', 'dom'), may hold values from 0.15 to 0.45
- fluid_coupling: float32 [4, 256, 128], P('grp', 'dom'), may hold values from 0.1 to 0.5
- solid_start: float32 [4, 128, 24, 128], P('grp', 'dom'), may hold values from -6 to 6
- solid_rate: float32 [4, 128, 24, 128], P('grp', 'dom'), may hold values from 0.2 to 0.6
- solid_coupling: float32 [4, 128, 128], P('grp', 'dom'), may hold values from 0.1 to 0.5
- solid_block: int32 [3072], P(('grp', 'dom')), may hold values from 0 to 127, as said below
- to_solid: bfloat16 [3072, 128, 128], P(('grp', 'dom')), as said below
- to_fluid: bfloat16 [3072, 128, 128], P(('grp', 'dom')), as said below
Outputs:
- fluid_temp: float32 [4, 256, 96, 128], P('grp', 'dom')
- solid_temp: float32 [4, 128, 24, 128], P('grp', 'dom')
The draws below stay inside these ranges and needn't reach their ends.
Inputs may be any that keep to these rules, and one draw needn't show every extreme that they name: For segment s of fluid block x of its zone (x = (s // 3) mod 256), solid_block[s] lies within x // 2 - 2 to x // 2 + 2, taken modulo 128. `to_solid`: entry [s, i, j] is zero unless i and j differ by at most one; all entries are nonnegative. `to_fluid`: entry [s, i, j] is zero unless i and j differ by at most one; all entries are nonnegative.
All inputs are finite; a program needn't handle non-finite values.
Results may differ from the reference program's by a relative error of at most 0.0003.
Values may be sent and summed in bfloat16 or wider, within the bound.
A program may use at most 128 MiB of HBM per device.

```python
import math
import jax
import jax.numpy as jnp
from jax import lax

FX = 32
FY = 96
FZ = 128
SX = 16
SEG_BLOCK = 3
PICARD = 4
SWEEPS = 2
SY = 24
SEG_DEV = 96
NXF = 256
NXS = 128
NFB = 1024
NSEG = 3072
N_GRP = 4
N_DOM = 8


def parity_pattern(shape):
    along_x = lax.broadcasted_iota(jnp.int32, shape, 1)
    along_y = lax.broadcasted_iota(jnp.int32, shape, 2)
    along_z = lax.broadcasted_iota(jnp.int32, shape, 3)
    return (1 - 2 * ((along_x + along_y + along_z) % 2)).astype(jnp.float32)


def draw_fluid_start(key, part):
    shape = (N_GRP, NXF, FY, FZ)
    inner_key = jax.random.fold_in(key, 41)
    magnitude = jnp.clip(2.0 + 0.8 * jax.random.normal(inner_key, shape, jnp.float32), 0.25, 5.0)
    return (parity_pattern(shape) * magnitude).astype(jnp.float32)


def draw_solid_start(key, part):
    shape = (N_GRP, NXS, SY, FZ)
    inner_key = jax.random.fold_in(key, 43)
    magnitude = jnp.clip(2.0 + 0.8 * jax.random.normal(inner_key, shape, jnp.float32), 0.25, 5.0)
    return (parity_pattern(shape) * magnitude).astype(jnp.float32)


def draw_solid_block(key, part):
    jitter = jax.random.randint(jax.random.fold_in(key, 11), (NFB,), 0, 3).astype(jnp.int32)
    position = jnp.arange(NFB, dtype=jnp.int32) % NXF
    within = position % FX
    jitter = jnp.where(within == 0, 0, jnp.where(within == FX - 1, 2, jitter)).astype(jnp.int32)
    lowest = position // 2 + jitter - 2
    spread = lowest[:, None] + jnp.arange(SEG_BLOCK, dtype=jnp.int32)[None, :]
    return (spread % NXS).reshape(-1).astype(jnp.int32)


def intersect_fractions(key):
    shares = jax.random.uniform(jax.random.fold_in(key, 5), (NSEG // SEG_BLOCK, SEG_BLOCK), jnp.float32, 0.5, 1.5)
    return (shares / jnp.sum(shares, axis=1, keepdims=True)).reshape(-1)


def banded(key, salt):
    fractions = intersect_fractions(key)
    main_key, upper_key, lower_key = jax.random.split(jax.random.fold_in(key, salt), 3)
    centre = jax.random.uniform(main_key, (NSEG, FZ), jnp.float32, 1.0, 2.0)
    upper = jax.random.uniform(upper_key, (NSEG, FZ), jnp.float32, 0.2, 0.5)
    lower = jax.random.uniform(lower_key, (NSEG, FZ), jnp.float32, 0.2, 0.5)
    column = jnp.arange(FZ, dtype=jnp.int32)[None, :]
    upper = jnp.where(column >= 1, upper, 0.0)
    lower = jnp.where(column <= FZ - 2, lower, 0.0)
    scaling = fractions[:, None] / (centre + upper + lower)
    centre = centre * scaling
    upper = upper * scaling
    lower = lower * scaling

    def build(pieces):
        centre_part, upper_part, lower_part = pieces
        rows = lax.broadcasted_iota(jnp.int32, (FZ, FZ), 0)
        cols = lax.broadcasted_iota(jnp.int32, (FZ, FZ), 1)
        matrix = jnp.where(rows == cols, centre_part[:, None, :], jnp.where(rows == cols - 1, upper_part[:, None, :], jnp.where(rows == cols + 1, lower_part[:, None, :], 0.0)))
        return matrix.astype(jnp.bfloat16)
    groups = NSEG // SEG_DEV
    built = lax.map(build, (centre.reshape(groups, SEG_DEV, FZ), upper.reshape(groups, SEG_DEV, FZ), lower.reshape(groups, SEG_DEV, FZ)))
    return built.reshape(NSEG, FZ, FZ)


def draw_to_solid(key, part):
    return banded(key, 21)


def draw_to_fluid(key, part):
    return banded(key, 23)


def shard_levels(key, dims, cuts, least, top_value):
    gain, own = 1.0, jax.random.fold_in(key, 6)
    for dim, shards_of in cuts:
        draws = jnp.exp(jax.random.uniform(jax.random.fold_in(own, dim), (shards_of,), jnp.float32, least / len(cuts), top_value / len(cuts)))
        gain = gain * jnp.repeat(draws, dims[dim] // shards_of).reshape([-1 if axis == dim else 1 for axis in range(len(dims))])
    return gain


def setup_inputs(seed: int = 0) -> dict:
    streams_of = jax.random.split(jax.random.key(seed), 10)
    return {
        "fluid_start": draw_fluid_start(jax.random.fold_in(streams_of[9], 71), 0),
        "fluid_rate": jnp.clip(jnp.exp(math.log(0.45) - 1.0986122 * jax.random.uniform(streams_of[1], (N_GRP, NXF, FY, FZ), jnp.float32) ** shard_levels(streams_of[1], (N_GRP, NXF, FY, FZ), ((0, 4), (1, 8)), -0.2, 0.2)), 0.15, 0.45),
        "fluid_coupling": jnp.clip(jnp.exp(math.log(0.5) - 1.609438 * jax.random.uniform(streams_of[2], (N_GRP, NXF, FZ), jnp.float32) ** shard_levels(streams_of[2], (N_GRP, NXF, FZ), ((0, 4), (1, 8)), -0.2, 0.2)), 0.1, 0.5),
        "solid_start": draw_solid_start(jax.random.fold_in(streams_of[9], 71), 0),
        "solid_rate": jnp.clip(jnp.exp(math.log(0.6) - 1.0986123 * jax.random.uniform(streams_of[4], (N_GRP, NXS, SY, FZ), jnp.float32) ** shard_levels(streams_of[4], (N_GRP, NXS, SY, FZ), ((0, 4), (1, 8)), -0.2, 0.2)), 0.2, 0.6),
        "solid_coupling": jnp.clip(jnp.exp(math.log(0.5) - 1.609438 * jax.random.uniform(streams_of[5], (N_GRP, NXS, FZ), jnp.float32) ** shard_levels(streams_of[5], (N_GRP, NXS, FZ), ((0, 4), (1, 8)), -0.2, 0.2)), 0.1, 0.5),
        "solid_block": draw_solid_block(jax.random.fold_in(streams_of[9], 71), 0),
        "to_solid": draw_to_solid(jax.random.fold_in(streams_of[9], 71), 0),
        "to_fluid": draw_to_fluid(jax.random.fold_in(streams_of[9], 71), 0),
    }


def neighbours(field_now):
    padded = jnp.pad(field_now, ((0, 0), (1, 1), (1, 1), (1, 1)))
    summed = padded[:, 2:, 1:-1, 1:-1] + padded[:, :-2, 1:-1, 1:-1]
    summed = summed + padded[:, 1:-1, 2:, 1:-1] + padded[:, 1:-1, :-2, 1:-1]
    summed = summed + padded[:, 1:-1, 1:-1, 2:] + padded[:, 1:-1, 1:-1, :-2]
    return summed


def relax(summed, base_value, rate_value, film_value, incoming, plane_row):
    numerator = base_value + rate_value * summed
    denominator = 1.0 + 6.0 * rate_value
    numerator = numerator.at[:, :, plane_row, :].add(film_value * incoming)
    denominator = denominator.at[:, :, plane_row, :].add(film_value)
    return numerator / denominator


def reference(fluid_start, fluid_rate, fluid_coupling, solid_start, solid_rate, solid_coupling, solid_block, to_solid, to_fluid):
    devices = N_GRP * N_DOM
    fluid_blocks = devices * FX
    solid_blocks = devices * SX
    seg_ids = jnp.arange(NSEG, dtype=jnp.int32)
    fluid_ids = seg_ids // SEG_BLOCK
    zone_ids = seg_ids // (SEG_DEV * N_DOM)
    solid_ids = ((zone_ids + 1) % N_GRP) * NXS + solid_block
    fluid_now = fluid_start
    solid_now = solid_start
    for iteration in range(PICARD):
        fluid_face = fluid_now[:, :, 0, :].reshape(fluid_blocks, FZ).astype(jnp.bfloat16)
        solid_face = solid_now[:, :, -1, :].reshape(solid_blocks, FZ).astype(jnp.bfloat16)

        def project(pieces):
            fluid_part, solid_part, solid_mats, fluid_mats = pieces
            solid_terms = jnp.einsum("sk,skm->sm", fluid_face[fluid_part].astype(jnp.float32), solid_mats.astype(jnp.float32))
            fluid_terms = jnp.einsum("sk,skm->sm", solid_face[solid_part].astype(jnp.float32), fluid_mats.astype(jnp.float32))
            return solid_terms, fluid_terms

        solid_terms, fluid_terms = lax.map(project, (
            fluid_ids.reshape(devices, SEG_DEV),
            solid_ids.reshape(devices, SEG_DEV),
            to_solid.reshape(devices, SEG_DEV, FZ, FZ),
            to_fluid.reshape(devices, SEG_DEV, FZ, FZ)))
        solid_in = jax.ops.segment_sum(solid_terms.reshape(-1, FZ), solid_ids, num_segments=solid_blocks)
        fluid_in = jax.ops.segment_sum(fluid_terms.reshape(-1, FZ), fluid_ids, num_segments=fluid_blocks)
        solid_in = solid_in.reshape(N_GRP, NXS, FZ)
        fluid_in = fluid_in.reshape(N_GRP, NXF, FZ)
        for sweep_no in range(SWEEPS):
            fluid_now = relax(neighbours(fluid_now), fluid_start, fluid_rate, fluid_coupling, fluid_in, 0)
            solid_now = relax(neighbours(solid_now), solid_start, solid_rate, solid_coupling, solid_in, -1)
    return fluid_now, solid_now
```

```python
import functools

import jax
import jax.numpy as jnp
from jax import lax
from jax.experimental import pallas as pl
from jax.experimental.pallas import tpu as pltpu
from jax.sharding import PartitionSpec as P

PICARD = 4
CHUNKS = 4
MESH = pl.DeviceIdType.MESH
F32 = jnp.float32
BF16 = jnp.bfloat16


def body(
    n_grp, n_dom, per_block,
    fs, fr, fc, ss, sr, sc, off, ts, tf,
    fo, so,
    U0, U1, A, B, CPL, CF, Q,
    V0, V1, AS, BS, SCP, CFS, QS,
    MS, MF, WF, WS,
    PB, GB, LP0, LP1, LP2, LG, LGS, HF, HS,
    lsem, msem, s_init, r_init, s_row, r_row, s_face, r_face,
):
    g = lax.axis_index("grp")
    d = lax.axis_index("dom")
    R, Y = fs.shape[1], fs.shape[2]
    K, SY = ss.shape[1], ss.shape[2]
    dr = lax.rem(d + 1, n_dom)
    dl = lax.rem(d + n_dom - 1, n_dom)
    gu = lax.rem(g + 1, n_grp)
    gd = lax.rem(g + n_grp - 1, n_grp)
    has_r = d < n_dom - 1
    has_l = d > 0

    own = [
        (fs.at[0], U0.at[2 : R + 2, 8 : Y + 8]),
        (fr.at[0], B.at[2 : R + 2]),
        (fc.at[0], CPL.at[8 : R + 8]),
        (ss.at[0], V0.at[2 : K + 2, 8 : SY + 8]),
        (sr.at[0], BS.at[2 : K + 2]),
        (sc.at[0], SCP.at[8 : K + 8]),
    ]
    own = [pltpu.make_async_copy(a, b, lsem.at[i]) for i, (a, b) in enumerate(own)]
    for c in own:
        c.start()
    seg = ts.shape[0]
    part = seg // CHUNKS
    mats = []
    for q in range(CHUNKS):
        rows = pl.ds(q * part, part)
        mats.append(
            (
                pltpu.make_async_copy(tf.at[rows], MF.at[rows], msem.at[0, q]),
                pltpu.make_async_copy(ts.at[rows], MS.at[rows], msem.at[1, q]),
            )
        )
        for c in mats[-1]:
            c.start()

    for U, rows, wide in ((U0, R, Y), (U1, R, Y), (V0, K, SY), (V1, K, SY)):
        U[:, 0:8, :] = jnp.zeros((rows + 4, 8, 128), F32)
        U[:, wide + 8 : wide + 16, :] = jnp.zeros((rows + 4, 8, 128), F32)
    for U, rows, wide in ((U0, R, Y), (V0, K, SY)):
        U[0:2, 8 : wide + 8, :] = jnp.zeros((2, wide, 128), F32)
        U[rows + 2 : rows + 4, 8 : wide + 8, :] = jnp.zeros((2, wide, 128), F32)
    for U, rows, wide in ((B, R, Y), (BS, K, SY)):
        U[1, :, :] = jnp.zeros((wide, 128), F32)
        U[rows + 2, :, :] = jnp.zeros((wide, 128), F32)
    for C, rows in ((CPL, R), (SCP, K)):
        C[0:8, :] = jnp.zeros((8, 128), F32)
        C[rows + 8 : rows + 16, :] = jnp.zeros((8, 128), F32)
    CF[...] = jnp.zeros(CF.shape, F32)
    CFS[...] = jnp.zeros(CFS.shape, F32)
    WF[0] = jnp.zeros(WF.shape[1:], F32)
    WF[K + 1] = jnp.zeros(WF.shape[1:], F32)
    PB[...] = jnp.zeros(PB.shape, F32)

    barrier = pltpu.get_barrier_semaphore()
    around = [(g, dr), (g, dl)] + [(z, x) for z in (gu, gd) for x in (dl, d, dr)]
    for dev in around:
        pl.semaphore_signal(barrier, inc=1, device_id=dev, device_id_type=MESH)
    pl.semaphore_wait(barrier, len(around))

    def remote(src, dst, ssem, rsem, dev):
        return pltpu.make_async_remote_copy(
            src_ref=src, dst_ref=dst, send_sem=ssem, recv_sem=rsem,
            device_id=dev, device_id_type=MESH,
        )

    def init_list(side):
        if side == 0:
            dev, e, h = (g, dr), lambda n, w: pl.ds(n - w, w), lambda n, w, o: pl.ds(o - w, w)
        else:
            dev, e, h = (g, dl), lambda n, w: pl.ds(0, w), lambda n, w, o: pl.ds(n + o, w)
        pairs = [
            (fs.at[0, e(R, 2)], U0.at[h(R, 2, 2), 8 : Y + 8]),
            (fr.at[0, e(R, 1)], B.at[h(R, 1, 2)]),
            (fc.at[0, e(R, 8)], CPL.at[h(R, 8, 8)]),
            (ss.at[0, e(K, 2)], V0.at[h(K, 2, 2), 8 : SY + 8]),
            (sr.at[0, e(K, 1)], BS.at[h(K, 1, 2)]),
            (sc.at[0, e(K, 8)], SCP.at[h(K, 8, 8)]),
            (WF.at[K, 1], WF.at[0, 1]) if side == 0 else (WF.at[1, 0], WF.at[K + 1, 0]),
        ]
        return [
            remote(a, b, s_init.at[side, i], r_init.at[side, i], dev)
            for i, (a, b) in enumerate(pairs)
        ]

    inits = [init_list(0), init_list(1)]
    can_send = (has_r, has_l)
    can_recv = (has_l, has_r)

    for side in range(2):
        @pl.when(can_send[side])
        def _(side=side):
            for c in inits[side][:6]:
                c.start()

    lane = lax.broadcasted_iota(jnp.int32, (16, 128), 1)
    row16 = lax.broadcasted_iota(jnp.int32, (16, 128), 0)
    masks = [row16 == ((lane + t + 16) & 15) for t in (-1, 0, 1)]
    sub8 = lax.broadcasted_iota(jnp.int32, (8, 128), 0)

    def extract(c, _):
        for M, W, base in ((MF, WF, 1), (MS, WS, 0)):
            for p in range(2):
                acc = [jnp.zeros((8, 128), F32) for _ in range(3)]
                for k in range(per_block):
                    s = (2 * c + p) * per_block + k
                    folded = M[s, 0:16, :].astype(F32)
                    for r in range(1, 8):
                        folded = folded + M[s, 16 * r : 16 * r + 16, :].astype(F32)
                    at = sub8 == off[s]
                    for t in range(3):
                        line = jnp.sum(jnp.where(masks[t], folded, 0.0), axis=0, keepdims=True)
                        acc[t] = acc[t] + jnp.where(at, jnp.broadcast_to(line, (8, 128)), 0.0)
                for t in range(3):
                    W[c + base, p, t] = acc[t]
        return 0

    per = K // CHUNKS
    for q in range(CHUNKS):
        for c in mats[q]:
            c.wait()
        lax.fori_loop(q * per, (q + 1) * per, extract, 0)
    for side in range(2):
        @pl.when(can_send[side])
        def _(side=side):
            inits[side][6].start()
    for c in own:
        c.wait()

    def face_copies(i):
        sem = lambda j: (s_face.at[i, j], r_face.at[i, j])
        return [
            remote(GB.at[i], LG.at[i, 8 : K + 8], *sem(0), (gd, d)),
            remote(GB.at[i, K - 8 : K], LG.at[i, 0:8], *sem(1), (gd, dr)),
            remote(GB.at[i, 0:8], LG.at[i, K + 8 : K + 16], *sem(2), (gd, dl)),
            remote(PB.at[i], LP1.at[i], *sem(3), (gu, d)),
            remote(PB.at[i, K : K + 16], LP0.at[i], *sem(4), (gu, dr)),
            remote(PB.at[i, 0:16], LP2.at[i], *sem(5), (gu, dl)),
        ]

    def row_copies(i):
        sem = lambda s, j: (s_row.at[i - 1, s, j], r_row.at[i - 1, s, j])
        return [
            [
                remote(U0.at[R : R + 2, 8 : Y + 8], HF.at[i - 1, 0], *sem(0, 0), (g, dr)),
                remote(V0.at[K : K + 2, 8 : SY + 8], HS.at[i - 1, 0], *sem(0, 1), (g, dr)),
            ],
            [
                remote(U0.at[2:4, 8 : Y + 8], HF.at[i - 1, 1], *sem(1, 0), (g, dl)),
                remote(V0.at[2:4, 8 : SY + 8], HS.at[i - 1, 1], *sem(1, 1), (g, dl)),
            ],
        ]

    def build_solid_face(i):
        def step(c, _):
            line = V0[c + 2, SY + 7 : SY + 8, :]
            GB[i, pl.ds(c, 1), :] = line.astype(BF16).astype(F32)
            return 0
        lax.fori_loop(0, K, step, 0)

    def build_partial(i):
        def step(c, _):
            total = None
            for p in range(2):
                line = U0[2 * c + p + 2, 8:9, :].astype(BF16).astype(F32)
                wide = jnp.broadcast_to(line, (8, 128))
                views = (pltpu.roll(wide, 1, 1), wide, pltpu.roll(wide, 127, 1))
                for t in range(3):
                    term = views[t] * WS[c, p, t]
                    total = term if total is None else total + term
            PB[i, pl.ds(c + 6, 8), :] = PB[i, pl.ds(c + 6, 8), :] + total
            return 0
        lax.fori_loop(0, K, step, 0)

    def coefficients(U, X, Z, cpl, cf, wide, plane, first, last):
        at = lax.broadcasted_iota(jnp.int32, (wide, 128), 0) == plane
        def step(x, _):
            rate = Z[x]
            film = cpl[pl.ds(x + 6, 1), :]
            den = 1.0 + 6.0 * rate
            den = den + jnp.where(at, jnp.broadcast_to(film, (wide, 128)), 0.0)
            inv = 1.0 / den
            X[x] = U[x, 8 : wide + 8, :] * inv
            Z[x] = rate * inv
            cf[pl.ds(x + 6, 1), :] = film * inv[plane : plane + 1, :]
            return 0
        lax.fori_loop(first, last, step, 0)

    def sweep(src, dst, X, Z, wide, first, last):
        z = lax.broadcasted_iota(jnp.int32, (wide, 128), 1)
        at_l, at_r = z == 0, z == 127
        def step(x, _):
            c = src[x, 8 : wide + 8, :]
            s = src[x - 1, 8 : wide + 8, :] + src[x + 1, 8 : wide + 8, :]
            s = s + src[x, 7 : wide + 7, :] + src[x, 9 : wide + 9, :]
            s = s + jnp.where(at_l, 0.0, pltpu.roll(c, 1, 1))
            s = s + jnp.where(at_r, 0.0, pltpu.roll(c, 127, 1))
            dst[x, 8 : wide + 8, :] = X[x] + Z[x] * s
            return 0
        lax.fori_loop(first, last, step, 0)

    def patch(dst, q, row, first, last):
        def step(x, _):
            dst[x, row : row + 1, :] = dst[x, row : row + 1, :] + q[pl.ds(x + 6, 1), :]
            return 0
        lax.fori_loop(first, last, step, 0)

    coefficients(U0, A, B, CPL, CF, Y, 0, 2, R + 2)
    coefficients(V0, AS, BS, SCP, CFS, SY, SY - 1, 2, K + 2)

    for i in range(PICARD):
        build_solid_face(i)
        build_partial(i)
        faces = face_copies(i)
        for c in faces:
            c.start()
        rows = row_copies(i) if i else inits
        if i:
            for side in range(2):
                @pl.when(can_send[side])
                def _(side=side):
                    for c in rows[side]:
                        c.start()
        sweep(U0, U1, A, B, Y, 3, R + 1)
        sweep(V0, V1, AS, BS, SY, 3, K + 1)
        for side in range(2):
            @pl.when(can_recv[side])
            def _(side=side):
                for c in rows[side]:
                    c.wait_recv()
                if i:
                    at = 0 if side == 0 else R + 2
                    U0[at : at + 2, 8 : Y + 8, :] = HF[i - 1, side]
                    at = 0 if side == 0 else K + 2
                    V0[at : at + 2, 8 : SY + 8, :] = HS[i - 1, side]
        if i == 0:
            for at in (1, R + 2):
                coefficients(U0, A, B, CPL, CF, Y, 0, at, at + 1)
            for at in (1, K + 2):
                coefficients(V0, AS, BS, SCP, CFS, SY, SY - 1, at, at + 1)
        for first in (1, R + 1):
            sweep(U0, U1, A, B, Y, first, first + 2)
        for first in (1, K + 1):
            sweep(V0, V1, AS, BS, SY, first, first + 2)

        for c in faces[:3]:
            c.wait_recv()
        near = LG[i]
        LGS[0] = pltpu.roll(near, 1, 1)
        LGS[1] = near
        LGS[2] = pltpu.roll(near, 127, 1)

        def incoming(c, _):
            views = [LGS[t, pl.ds(c + 5, 8), :] for t in range(3)]
            for p in range(2):
                term = views[0] * WF[c, p, 0] + views[1] * WF[c, p, 1] + views[2] * WF[c, p, 2]
                line = jnp.sum(term, axis=0, keepdims=True)
                at = 2 * c + p + 6
                Q[pl.ds(at, 1), :] = CF[pl.ds(at, 1), :] * line
            return 0

        lax.fori_loop(0, K + 2, incoming, 0)
        patch(U1, Q, 8, 1, R + 3)
        for c in faces[3:]:
            c.wait_recv()
        QS[0:16, :] = CFS[0:16, :] * (LP1[i, 0:16, :] + LP0[i])
        QS[K : K + 16, :] = CFS[K : K + 16, :] * (LP1[i, K : K + 16, :] + LP2[i])
        patch(V1, QS, SY + 7, 1, K + 3)

        if i:
            for side in range(2):
                @pl.when(can_send[side])
                def _(side=side):
                    for c in rows[side]:
                        c.wait_send()
        sweep(U1, U0, A, B, Y, 2, R + 2)
        patch(U0, Q, 8, 2, R + 2)
        sweep(V1, V0, AS, BS, SY, 2, K + 2)
        patch(V0, QS, SY + 7, 2, K + 2)
        for c in faces:
            c.wait_send()

    for side in range(2):
        @pl.when(can_send[side])
        def _(side=side):
            for c in inits[side]:
                c.wait_send()
    outs = [
        pltpu.make_async_copy(U0.at[2 : R + 2, 8 : Y + 8], fo.at[0], lsem.at[0]),
        pltpu.make_async_copy(V0.at[2 : K + 2, 8 : SY + 8], so.at[0], lsem.at[1]),
    ]
    for c in outs:
        c.start()
    for c in outs:
        c.wait()


def local(n_grp, n_dom, fs, fr, fc, ss, sr, sc, blocks, ts, tf):
    R, Y = fs.shape[1], fs.shape[2]
    K, SY = ss.shape[1], ss.shape[2]
    seg = ts.shape[0]
    per_block = seg // R
    centre = K * lax.axis_index("dom") + jnp.arange(seg, dtype=jnp.int32) // (2 * per_block)
    off = (blocks - centre + 2) % (K * n_dom)
    v = lambda *s: pltpu.VMEM(s, F32)
    dma = lambda *s: pltpu.SemaphoreType.DMA(s)
    anyspec = pl.BlockSpec(memory_space=pl.ANY)
    return tuple(
        pl.pallas_call(
            functools.partial(body, n_grp, n_dom, per_block),
            out_shape=(
                jax.ShapeDtypeStruct(fs.shape, F32),
                jax.ShapeDtypeStruct(ss.shape, F32),
            ),
            in_specs=[anyspec] * 6 + [pl.BlockSpec(memory_space=pltpu.SMEM)] + [anyspec] * 2,
            out_specs=(anyspec, anyspec),
            scratch_shapes=[
                v(R + 4, Y + 16, 128), v(R + 4, Y + 16, 128), v(R + 4, Y, 128), v(R + 4, Y, 128),
                v(R + 16, 128), v(R + 16, 128), v(R + 16, 128),
                v(K + 4, SY + 16, 128), v(K + 4, SY + 16, 128), v(K + 4, SY, 128), v(K + 4, SY, 128),
                v(K + 16, 128), v(K + 16, 128), v(K + 16, 128),
                pltpu.VMEM(ts.shape, BF16), pltpu.VMEM(tf.shape, BF16),
                v(K + 2, 2, 3, 8, 128), v(K, 2, 3, 8, 128),
                v(PICARD, K + 16, 128), v(PICARD, K, 128),
                v(PICARD, 16, 128), v(PICARD, K + 16, 128), v(PICARD, 16, 128),
                v(PICARD, K + 16, 128), v(3, K + 16, 128),
                v(PICARD - 1, 2, 2, Y, 128), v(PICARD - 1, 2, 2, SY, 128),
                dma(6), dma(2, CHUNKS), dma(2, 7), dma(2, 7),
                dma(PICARD - 1, 2, 2), dma(PICARD - 1, 2, 2), dma(PICARD, 6), dma(PICARD, 6),
            ],
            compiler_params=pltpu.CompilerParams(collective_id=0, has_side_effects=True),
            name="cht",
        )(fs, fr, fc, ss, sr, sc, off, ts, tf)
    )


def solution(mesh):
    zone = P("grp", "dom", None, None)
    face = P("grp", "dom", None)
    flat = P(("grp", "dom"), None, None)
    return jax.shard_map(
        functools.partial(local, mesh.shape["grp"], mesh.shape["dom"]),
        mesh=mesh,
        in_specs=(zone, zone, face, zone, zone, face, P(("grp", "dom")), flat, flat),
        out_specs=(zone, zone),
        check_vma=False,
    )
```

```python
import functools

import jax
import jax.numpy as jnp
from jax import lax
from jax.experimental import pallas as pl
from jax.experimental.pallas import tpu as pltpu
from jax.sharding import PartitionSpec as P

PICARD = 4
CHUNKS = 4
UNROLL = 4
MESH = pl.DeviceIdType.MESH
F32 = jnp.float32
BF16 = jnp.bfloat16


def loop(first, last, unroll, step):
    trips = (last - first) // unroll
    def many(i, _):
        for j in range(unroll):
            step(first + i * unroll + j)
        return 0
    if trips > 1:
        lax.fori_loop(0, trips, many, 0)
    elif trips == 1:
        many(0, 0)
    for x in range(first + trips * unroll, last):
        step(x)


def body(
    n_grp, n_dom, per_block,
    fs, fr, fc, ss, sr, sc, off, ts, tf,
    fo, so,
    U0, U1, A, B, CPL, CF, Q,
    V0, V1, AS, BS, SCP, CFS, QS,
    MS, MF, WF, WS,
    PB, GB, FB, FS, LP0, LP1, LP2, LG, LGS, HF, HS,
    lsem, msem, s_init, r_init, s_row, r_row, s_face, r_face,
):
    g = lax.axis_index("grp")
    d = lax.axis_index("dom")
    R, Y = fs.shape[1], fs.shape[2]
    K, SY = ss.shape[1], ss.shape[2]
    dr = lax.rem(d + 1, n_dom)
    dl = lax.rem(d + n_dom - 1, n_dom)
    gu = lax.rem(g + 1, n_grp)
    gd = lax.rem(g + n_grp - 1, n_grp)
    has_r = d < n_dom - 1
    has_l = d > 0

    own = [
        (fs.at[0], U0.at[2 : R + 2, 8 : Y + 8]),
        (fr.at[0], B.at[2 : R + 2]),
        (fc.at[0], CPL.at[8 : R + 8]),
        (ss.at[0], V0.at[2 : K + 2, 8 : SY + 8]),
        (sr.at[0], BS.at[2 : K + 2]),
        (sc.at[0], SCP.at[8 : K + 8]),
    ]
    own = [pltpu.make_async_copy(a, b, lsem.at[i]) for i, (a, b) in enumerate(own)]
    for c in own:
        c.start()
    seg = ts.shape[0]
    part = seg // CHUNKS
    mats = []
    for q in range(CHUNKS):
        rows = pl.ds(q * part, part)
        mats.append(
            (
                pltpu.make_async_copy(tf.at[rows], MF.at[rows], msem.at[0, q]),
                pltpu.make_async_copy(ts.at[rows], MS.at[rows], msem.at[1, q]),
            )
        )
        for c in mats[-1]:
            c.start()

    for U, rows, wide in ((U0, R, Y), (U1, R, Y), (V0, K, SY), (V1, K, SY)):
        U[:, 0:8, :] = jnp.zeros((rows + 4, 8, 128), F32)
        U[:, wide + 8 : wide + 16, :] = jnp.zeros((rows + 4, 8, 128), F32)
    for U, rows, wide in ((U0, R, Y), (V0, K, SY)):
        U[0:2, 8 : wide + 8, :] = jnp.zeros((2, wide, 128), F32)
        U[rows + 2 : rows + 4, 8 : wide + 8, :] = jnp.zeros((2, wide, 128), F32)
    for U, rows, wide in ((B, R, Y), (BS, K, SY)):
        U[1, :, :] = jnp.zeros((wide, 128), F32)
        U[rows + 2, :, :] = jnp.zeros((wide, 128), F32)
    for C, rows in ((CPL, R), (SCP, K)):
        C[0:8, :] = jnp.zeros((8, 128), F32)
        C[rows + 8 : rows + 16, :] = jnp.zeros((8, 128), F32)
    CF[...] = jnp.zeros(CF.shape, F32)
    CFS[...] = jnp.zeros(CFS.shape, F32)
    WF[0] = jnp.zeros(WF.shape[1:], F32)
    WF[K + 1] = jnp.zeros(WF.shape[1:], F32)
    PB[...] = jnp.zeros(PB.shape, F32)

    barrier = pltpu.get_barrier_semaphore()
    around = [(g, dr), (g, dl)] + [(z, x) for z in (gu, gd) for x in (dl, d, dr)]
    for dev in around:
        pl.semaphore_signal(barrier, inc=1, device_id=dev, device_id_type=MESH)
    pl.semaphore_wait(barrier, len(around))

    def remote(src, dst, ssem, rsem, dev):
        return pltpu.make_async_remote_copy(
            src_ref=src, dst_ref=dst, send_sem=ssem, recv_sem=rsem,
            device_id=dev, device_id_type=MESH,
        )

    def init_list(side):
        if side == 0:
            dev, e, h = (g, dr), lambda n, w: pl.ds(n - w, w), lambda n, w, o: pl.ds(o - w, w)
        else:
            dev, e, h = (g, dl), lambda n, w: pl.ds(0, w), lambda n, w, o: pl.ds(n + o, w)
        pairs = [
            (fs.at[0, e(R, 2)], U0.at[h(R, 2, 2), 8 : Y + 8]),
            (fr.at[0, e(R, 1)], B.at[h(R, 1, 2)]),
            (fc.at[0, e(R, 8)], CPL.at[h(R, 8, 8)]),
            (ss.at[0, e(K, 2)], V0.at[h(K, 2, 2), 8 : SY + 8]),
            (sr.at[0, e(K, 1)], BS.at[h(K, 1, 2)]),
            (sc.at[0, e(K, 8)], SCP.at[h(K, 8, 8)]),
            (WF.at[K, 1], WF.at[0, 1]) if side == 0 else (WF.at[1, 0], WF.at[K + 1, 0]),
        ]
        return [
            remote(a, b, s_init.at[side, i], r_init.at[side, i], dev)
            for i, (a, b) in enumerate(pairs)
        ]

    inits = [init_list(0), init_list(1)]
    can_send = (has_r, has_l)
    can_recv = (has_l, has_r)

    for side in range(2):
        @pl.when(can_send[side])
        def _(side=side):
            for c in inits[side][:6]:
                c.start()

    lane = lax.broadcasted_iota(jnp.int32, (16, 128), 1)
    row16 = lax.broadcasted_iota(jnp.int32, (16, 128), 0)
    masks = [row16 == ((lane + t + 16) & 15) for t in (-1, 0, 1)]
    sub8 = lax.broadcasted_iota(jnp.int32, (8, 128), 0)

    def extract(c, _):
        for M, W, base in ((MF, WF, 1), (MS, WS, 0)):
            for p in range(2):
                acc = [jnp.zeros((8, 128), F32) for _ in range(3)]
                for k in range(per_block):
                    s = (2 * c + p) * per_block + k
                    folded = M[s, 0:16, :]
                    for r in range(1, 8):
                        folded = folded + M[s, 16 * r : 16 * r + 16, :]
                    folded = folded.astype(F32)
                    at = sub8 == lax.rem(off[s] - (K * d + c) + 2 + K * n_dom, K * n_dom)
                    for t in range(3):
                        line = jnp.sum(jnp.where(masks[t], folded, 0.0), axis=0, keepdims=True)
                        acc[t] = acc[t] + jnp.where(at, jnp.broadcast_to(line, (8, 128)), 0.0)
                for t in range(3):
                    W[c + base, p, t] = acc[t]
        return 0

    per = K // CHUNKS
    for q in range(CHUNKS):
        for c in mats[q]:
            c.wait()
        lax.fori_loop(q * per, (q + 1) * per, extract, 0)
    for side in range(2):
        @pl.when(can_send[side])
        def _(side=side):
            inits[side][6].start()
    for c in own:
        c.wait()

    def face_copies(i):
        sem = lambda j: (s_face.at[i, j], r_face.at[i, j])
        return [
            remote(GB.at[i], LG.at[i, 8 : K + 8], *sem(0), (gd, d)),
            remote(GB.at[i, K - 8 : K], LG.at[i, 0:8], *sem(1), (gd, dr)),
            remote(GB.at[i, 0:8], LG.at[i, K + 8 : K + 16], *sem(2), (gd, dl)),
            remote(PB.at[i], LP1.at[i], *sem(3), (gu, d)),
            remote(PB.at[i, K : K + 16], LP0.at[i], *sem(4), (gu, dr)),
            remote(PB.at[i, 0:16], LP2.at[i], *sem(5), (gu, dl)),
        ]

    def row_copies(i):
        sem = lambda s, j: (s_row.at[i - 1, s, j], r_row.at[i - 1, s, j])
        return [
            [
                remote(U0.at[R : R + 2, 8 : Y + 8], HF.at[i - 1, 0], *sem(0, 0), (g, dr)),
                remote(V0.at[K : K + 2, 8 : SY + 8], HS.at[i - 1, 0], *sem(0, 1), (g, dr)),
            ],
            [
                remote(U0.at[2:4, 8 : Y + 8], HF.at[i - 1, 1], *sem(1, 0), (g, dl)),
                remote(V0.at[2:4, 8 : SY + 8], HS.at[i - 1, 1], *sem(1, 1), (g, dl)),
            ],
        ]

    def build_solid_face(i):
        for c in range(K):
            line = V0[c + 2, SY + 7 : SY + 8, :]
            GB[i, c : c + 1, :] = line.astype(BF16).astype(F32)

    def build_partial(i):
        for c in range(K):
            for p in range(2):
                FB[p, c : c + 1, :] = U0[2 * c + p + 2, 8:9, :]
        for p in range(2):
            line = FB[p].astype(BF16).astype(F32)
            FS[0, p] = pltpu.roll(line, 1, 1)
            FS[1, p] = line
            FS[2, p] = pltpu.roll(line, 127, 1)
        for c in range(K):
            total = None
            for p in range(2):
                for t in range(3):
                    wide = jnp.broadcast_to(FS[t, p, c : c + 1, :], (8, 128))
                    term = wide * WS[c, p, t]
                    total = term if total is None else total + term
            PB[i, c + 6 : c + 14, :] = PB[i, c + 6 : c + 14, :] + total

    def coefficients(U, X, Z, cpl, cf, wide, plane, first, last):
        at = lax.broadcasted_iota(jnp.int32, (wide, 128), 0) == plane
        def step(x):
            rate = Z[x]
            film = cpl[pl.ds(x + 6, 1), :]
            den = 1.0 + 6.0 * rate
            den = den + jnp.where(at, jnp.broadcast_to(film, (wide, 128)), 0.0)
            inv = 1.0 / den
            X[x] = U[x, 8 : wide + 8, :] * inv
            Z[x] = rate * inv
            cf[pl.ds(x + 6, 1), :] = film * inv[plane : plane + 1, :]
        loop(first, last, 2, step)

    def sweep(src, dst, X, Z, wide, first, last, q=None, plane=0):
        z = lax.broadcasted_iota(jnp.int32, (wide, 128), 1)
        at_l, at_r = z == 0, z == 127
        tile = plane // 8 * 8
        at = lax.broadcasted_iota(jnp.int32, (8, 128), 0) == plane - tile
        def step(x):
            c = src[x, 8 : wide + 8, :]
            s = src[x - 1, 8 : wide + 8, :] + src[x + 1, 8 : wide + 8, :]
            s = s + src[x, 7 : wide + 7, :] + src[x, 9 : wide + 9, :]
            s = s + jnp.where(at_l, 0.0, pltpu.roll(c, 1, 1))
            s = s + jnp.where(at_r, 0.0, pltpu.roll(c, 127, 1))
            out = X[x] + Z[x] * s
            if q is None:
                dst[x, 8 : wide + 8, :] = out
            else:
                line = jnp.broadcast_to(q[pl.ds(x + 6, 1), :], (8, 128))
                piece = out[tile : tile + 8] + jnp.where(at, line, 0.0)
                if tile:
                    dst[x, 8 : tile + 8, :] = out[:tile]
                dst[x, tile + 8 : tile + 16, :] = piece
                if tile + 8 < wide:
                    dst[x, tile + 16 : wide + 8, :] = out[tile + 8 :]
        loop(first, last, UNROLL, step)

    def patch(dst, q, row, first, last):
        for low in range(first, last, 8):
            some = range(low, min(low + 8, last))
            new = [dst[x, row : row + 1, :] + q[x + 6 : x + 7, :] for x in some]
            for x, line in zip(some, new):
                dst[x, row : row + 1, :] = line

    coefficients(U0, A, B, CPL, CF, Y, 0, 2, R + 2)
    coefficients(V0, AS, BS, SCP, CFS, SY, SY - 1, 2, K + 2)

    for i in range(PICARD):
        build_solid_face(i)
        build_partial(i)
        faces = face_copies(i)
        for c in faces:
            c.start()
        rows = row_copies(i) if i else inits
        sweep(U0, U1, A, B, Y, 3, R + 1)
        sweep(V0, V1, AS, BS, SY, 3, K + 1)
        for side in range(2):
            @pl.when(can_recv[side])
            def _(side=side):
                for c in rows[side]:
                    c.wait_recv()
                if i:
                    at = 0 if side == 0 else R + 2
                    U0[at : at + 2, 8 : Y + 8, :] = HF[i - 1, side]
                    at = 0 if side == 0 else K + 2
                    V0[at : at + 2, 8 : SY + 8, :] = HS[i - 1, side]
        if i == 0:
            for at in (1, R + 2):
                coefficients(U0, A, B, CPL, CF, Y, 0, at, at + 1)
            for at in (1, K + 2):
                coefficients(V0, AS, BS, SCP, CFS, SY, SY - 1, at, at + 1)
        for first in (1, R + 1):
            sweep(U0, U1, A, B, Y, first, first + 2)
        for first in (1, K + 1):
            sweep(V0, V1, AS, BS, SY, first, first + 2)

        for c in faces[:3]:
            c.wait_recv()
        near = LG[i]
        LGS[0] = pltpu.roll(near, 1, 1)
        LGS[1] = near
        LGS[2] = pltpu.roll(near, 127, 1)

        def incoming(c):
            views = [LGS[t, pl.ds(c + 5, 8), :] for t in range(3)]
            for p in range(2):
                term = views[0] * WF[c, p, 0] + views[1] * WF[c, p, 1] + views[2] * WF[c, p, 2]
                line = jnp.sum(term, axis=0, keepdims=True)
                at = 2 * c + p + 6
                Q[pl.ds(at, 1), :] = CF[pl.ds(at, 1), :] * line

        loop(0, K + 2, 6, incoming)
        patch(U1, Q, 8, 1, R + 3)
        for c in faces[3:]:
            c.wait_recv()
        QS[0:16, :] = CFS[0:16, :] * (LP1[i, 0:16, :] + LP0[i])
        QS[K : K + 16, :] = CFS[K : K + 16, :] * (LP1[i, K : K + 16, :] + LP2[i])
        patch(V1, QS, SY + 7, 1, K + 3)

        if i:
            for side in range(2):
                @pl.when(can_send[side])
                def _(side=side):
                    for c in rows[side]:
                        c.wait_send()
        for first in (2, R):
            sweep(U1, U0, A, B, Y, first, first + 2, Q, 0)
        sweep(V1, V0, AS, BS, SY, 2, K + 2, QS, SY - 1)
        if i + 1 < PICARD:
            ahead = row_copies(i + 1)
            for side in range(2):
                @pl.when(can_send[side])
                def _(side=side):
                    for c in ahead[side]:
                        c.start()
        sweep(U1, U0, A, B, Y, 4, R, Q, 0)
        for c in faces:
            c.wait_send()

    for side in range(2):
        @pl.when(can_send[side])
        def _(side=side):
            for c in inits[side]:
                c.wait_send()
    outs = [
        pltpu.make_async_copy(U0.at[2 : R + 2, 8 : Y + 8], fo.at[0], lsem.at[0]),
        pltpu.make_async_copy(V0.at[2 : K + 2, 8 : SY + 8], so.at[0], lsem.at[1]),
    ]
    for c in outs:
        c.start()
    for c in outs:
        c.wait()


def local(n_grp, n_dom, fs, fr, fc, ss, sr, sc, blocks, ts, tf):
    R, Y = fs.shape[1], fs.shape[2]
    K, SY = ss.shape[1], ss.shape[2]
    seg = ts.shape[0]
    per_block = seg // R
    v = lambda *s: pltpu.VMEM(s, F32)
    dma = lambda *s: pltpu.SemaphoreType.DMA(s)
    anyspec = pl.BlockSpec(memory_space=pl.ANY)
    return tuple(
        pl.pallas_call(
            functools.partial(body, n_grp, n_dom, per_block),
            out_shape=(
                jax.ShapeDtypeStruct(fs.shape, F32),
                jax.ShapeDtypeStruct(ss.shape, F32),
            ),
            in_specs=[anyspec] * 6 + [pl.BlockSpec(memory_space=pltpu.SMEM)] + [anyspec] * 2,
            out_specs=(anyspec, anyspec),
            scratch_shapes=[
                v(R + 4, Y + 16, 128), v(R + 4, Y + 16, 128), v(R + 4, Y, 128), v(R + 4, Y, 128),
                v(R + 16, 128), v(R + 16, 128), v(R + 16, 128),
                v(K + 4, SY + 16, 128), v(K + 4, SY + 16, 128), v(K + 4, SY, 128), v(K + 4, SY, 128),
                v(K + 16, 128), v(K + 16, 128), v(K + 16, 128),
                pltpu.VMEM(ts.shape, BF16), pltpu.VMEM(tf.shape, BF16),
                v(K + 2, 2, 3, 8, 128), v(K, 2, 3, 8, 128),
                v(PICARD, K + 16, 128), v(PICARD, K, 128),
                v(2, K, 128), v(3, 2, K, 128),
                v(PICARD, 16, 128), v(PICARD, K + 16, 128), v(PICARD, 16, 128),
                v(PICARD, K + 16, 128), v(3, K + 16, 128),
                v(PICARD - 1, 2, 2, Y, 128), v(PICARD - 1, 2, 2, SY, 128),
                dma(6), dma(2, CHUNKS), dma(2, 7), dma(2, 7),
                dma(PICARD - 1, 2, 2), dma(PICARD - 1, 2, 2), dma(PICARD, 6), dma(PICARD, 6),
            ],
            compiler_params=pltpu.CompilerParams(collective_id=0, has_side_effects=True),
            name="cht",
        )(fs, fr, fc, ss, sr, sc, blocks, ts, tf)
    )


def solution(mesh):
    zone = P("grp", "dom", None, None)
    face = P("grp", "dom", None)
    flat = P(("grp", "dom"), None, None)
    return jax.shard_map(
        functools.partial(local, mesh.shape["grp"], mesh.shape["dom"]),
        mesh=mesh,
        in_specs=(zone, zone, face, zone, zone, face, P(("grp", "dom")), flat, flat),
        out_specs=(zone, zone),
        check_vma=False,
    )
```
